32 devices in a mesh: rows: 4 (over z), tp: 4 (over y, x), unit: 2 (over core).
Axes of the slice: x: 2, y: 2, z: 4, core: 2. Of those that a mesh axis runs over, the one named last changes fastest.
Arguments:
- w_query: bfloat16 [5120, 4096], P(('unit', 'rows'), 'tp'), parts along dimension 0, may hold values from -0.125 to 0.125
- low_query: bfloat16 [5120, 64], P(('unit', 'rows')), parts along dimension 0, may hold values from -0.125 to 0.125
- high_query: bfloat16 [128, 4096], P('unit', 'tp'), parts along dimension 0, may hold values from -0.75 to 0.75
- w_key: bfloat16 [5120, 1024], P(('unit', 'rows'), 'tp'), parts along dimension 0, may hold values from -0.125 to 0.125
- low_key: bfloat16 [5120, 64], P(('unit', 'rows')), parts along dimension 0, may hold values from -0.125 to 0.125
- high_key: bfloat16 [128, 1024], P('unit', 'tp'), parts along dimension 0, may hold values from -0.75 to 0.75
- w_value: bfloat16 [5120, 1024], P(('unit', 'rows'), 'tp'), parts along dimension 0, may hold values from -0.125 to 0.125
- low_value: bfloat16 [5120, 64], P(('unit', 'rows')), parts along dimension 0, may hold values from -0.125 to 0.125
- high_value: bfloat16 [128, 1024], P('unit', 'tp'), parts along dimension 0, may hold values from -0.75 to 0.75
- w_mixed: bfloat16 [8192, 2560], P(('unit', 'tp'), 'rows'), parts along dimension 0, may hold values from -0.09375 to 0.09375
- low_mixed: bfloat16 [8192, 64], P(('unit', 'tp')), parts along dimension 0, may hold values from -0.09375 to 0.09375
- high_mixed: bfloat16 [128, 2560], P('unit', 'rows'), parts along dimension 0, may hold values from -0.75 to 0.75
- norm_train: float32 [5120], P(('unit', 'rows', 'tp')), parts along dimension 0, may hold values from 0.25 to 1.75
- norm_step: float32 [5120], P(('unit', 'rows', 'tp')), parts along dimension 0, may hold values from -0.3 to 0.3
Outputs:
- final_query: bfloat16 [5120, 4096], P('unit', 'tp'), parts along dimension 0
- final_key: bfloat16 [5120, 1024], P('unit', 'tp'), parts along dimension 0
- final_value: bfloat16 [5120, 1024], P('unit', 'tp'), parts along dimension 0
- final_mixed: bfloat16 [8192, 2560], P(('unit', 'tp')), parts along dimension 0
- serve_norm: bfloat16 [5120], P('unit'), parts along dimension 0
The draws below stay inside these ranges and needn't reach their ends.
There are 2 independent parts, one for each index of `unit`. The reference program is written for one: setup_inputs(seed, part) draws one part's arguments, and reference() takes and returns one part's arrays. A program takes and returns all parts, laid end to end along the dimension named above; each array names one. Nothing has to cross between parts.
All inputs are finite; a program needn't handle non-finite values.
Results may differ from the reference program's by a relative error of at most 0.001.
Values may be sent and summed in bfloat16 or wider, within the bound.
A program may use at most 128 MiB of HBM per device.

```python
import jax
import jax.numpy as jnp

D_MODEL = 2560
Q_DIM = 4096
KV_DIM = 1024
RANK = 64


def block_levels(own_key, dims, pieces, smallest, largest):
    gain, own = 1.0, jax.random.fold_in(own_key, 6)
    for position, parts in pieces:
        steps = jnp.exp(jax.random.uniform(jax.random.fold_in(own, position), (parts,), jnp.float32, smallest / len(pieces), largest / len(pieces)))
        gain = gain * jnp.repeat(steps, dims[position] // parts).reshape([-1 if axis == position else 1 for axis in range(len(dims))])
    return gain


def gaussian(stream_key, shape, deviation, limit, pieces=(), dtype=jnp.bfloat16):
    drawn = jax.random.normal(stream_key, shape, jnp.float32) * deviation
    if len(pieces) > 0:
        drawn = block_levels(stream_key, shape, pieces, -0.22, 0.18) * drawn
    return jnp.clip(drawn, min=-limit, max=limit).astype(dtype)


def setup_inputs(seed: int = 0, part: int = 0) -> dict:
    key_of = jax.random.split(jax.random.key(seed), 15)
    own_keys = jax.random.split(jax.random.fold_in(key_of[14], part), 15)
    return {
        "w_query": gaussian(own_keys[0], (D_MODEL, Q_DIM), D_MODEL ** -0.5, 0.125, ((0, 4), (1, 4))),
        "low_query": gaussian(own_keys[1], (D_MODEL, RANK), D_MODEL ** -0.5, 0.125, ((0, 4),)),
        "high_query": gaussian(own_keys[2], (RANK, Q_DIM), RANK ** -0.5, 0.75, ((1, 4),)),
        "w_key": gaussian(own_keys[3], (D_MODEL, KV_DIM), D_MODEL ** -0.5, 0.125, ((0, 4), (1, 4))),
        "low_key": gaussian(own_keys[4], (D_MODEL, RANK), D_MODEL ** -0.5, 0.125, ((0, 4),)),
        "high_key": gaussian(own_keys[5], (RANK, KV_DIM), RANK ** -0.5, 0.75, ((1, 4),)),
        "w_value": gaussian(own_keys[6], (D_MODEL, KV_DIM), D_MODEL ** -0.5, 0.125, ((0, 4), (1, 4))),
        "low_value": gaussian(own_keys[7], (D_MODEL, RANK), D_MODEL ** -0.5, 0.125, ((0, 4),)),
        "high_value": gaussian(own_keys[8], (RANK, KV_DIM), RANK ** -0.5, 0.75, ((1, 4),)),
        "w_mixed": gaussian(own_keys[9], (Q_DIM, D_MODEL), Q_DIM ** -0.5, 0.09375, ((0, 4), (1, 4))),
        "low_mixed": gaussian(own_keys[10], (Q_DIM, RANK), Q_DIM ** -0.5, 0.09375, ((0, 4),)),
        "high_mixed": gaussian(own_keys[11], (RANK, D_MODEL), RANK ** -0.5, 0.75, ((1, 4),)),
        "norm_train": jnp.clip(1.0 + 0.15 * jax.random.normal(own_keys[12], (D_MODEL,), jnp.float32), 0.25, 1.75),
        "norm_step": jnp.clip(jax.random.uniform(own_keys[13], (D_MODEL,), jnp.float32, -0.3, 0.3) * block_levels(own_keys[13], (D_MODEL,), ((0, 16),), -0.4, 0.0), -0.3, 0.3),
    }


mix_rate = 0.5


def reference(w_query, low_query, high_query, w_key, low_key, high_key, w_value, low_value, high_value, w_mixed, low_mixed, high_mixed, norm_train, norm_step):
    result_query = w_query.astype(jnp.float32) + mix_rate * jnp.dot(low_query, high_query, preferred_element_type=jnp.float32)
    result_key = w_key.astype(jnp.float32) + mix_rate * jnp.dot(low_key, high_key, preferred_element_type=jnp.float32)
    result_value = w_value.astype(jnp.float32) + mix_rate * jnp.dot(low_value, high_value, preferred_element_type=jnp.float32)
    result_mixed = w_mixed.astype(jnp.float32) + mix_rate * jnp.dot(low_mixed, high_mixed, preferred_element_type=jnp.float32)
    final_query = result_query.astype(jnp.bfloat16)
    final_key = result_key.astype(jnp.bfloat16)
    final_value = result_value.astype(jnp.bfloat16)
    final_mixed = result_mixed.astype(jnp.bfloat16)
    serve_norm = (norm_train + norm_step).astype(jnp.bfloat16)
    return final_query, final_key, final_value, final_mixed, serve_norm
```

```python
import functools

import jax
import jax.numpy as jnp
from jax import lax
from jax.experimental import pallas as pl
from jax.experimental.pallas import tpu as pltpu
from jax.sharding import PartitionSpec as P

MESH = pl.DeviceIdType.MESH
mix_rate = 0.5
chunk_bytes = 400 * 1024


def pieces_of(rows, columns):
    count = 1
    while rows * columns * 2 > count * chunk_bytes and rows % (count * 32) == 0:
        count *= 2
    return count


def block_of(size, options):
    for option in options:
        if size % option == 0:
            return option
    return size


def kernel(n, tps, stacked, pieces, *refs):
    kinds = len(pieces)
    w, low, high = refs[:kinds], refs[kinds : 2 * kinds], refs[2 * kinds : 3 * kinds]
    norm_train, norm_step = refs[3 * kinds : 3 * kinds + 2]
    refs = refs[3 * kinds + 2 :]
    out, norm_out = refs[:kinds], refs[kinds]
    refs = refs[kinds + 1 :]
    w_own, low_own, high_own = refs[:kinds], refs[kinds : 2 * kinds], refs[2 * kinds : 3 * kinds]
    refs = refs[3 * kinds :]
    norm_all, load_sem, side_sem, send_sem, recv_sem, norm_send, norm_recv, cross_send, cross_recv = refs

    z, t = lax.axis_index("rows"), lax.axis_index("tp")
    chunks = [(k, p) for k in range(kinds) for p in range(pieces[k])]
    has_up, has_down = z < n - 1, z > 0

    barrier = pltpu.get_barrier_semaphore()

    @pl.when(has_up)
    def _():
        pl.semaphore_signal(barrier, inc=1, device_id={"rows": z + 1}, device_id_type=MESH)

    @pl.when(has_down)
    def _():
        pl.semaphore_signal(barrier, inc=1, device_id={"rows": z - 1}, device_id_type=MESH)

    for step in range(1, tps):
        pl.semaphore_signal(barrier, inc=1, device_id={"tp": lax.rem(t + step, tps)}, device_id_type=MESH)

    def rows_of(k, p):
        size = w[k].shape[0] // pieces[k]
        return p * size, size

    def load(i):
        k, p = chunks[i]
        start, size = rows_of(k, p)
        return pltpu.make_async_copy(
            w[k].at[pl.ds(start, size)], w_own[k].at[pl.ds(start, size)], load_sem.at[i]
        )

    def side(k):
        return (
            pltpu.make_async_copy(low[k], low_own[k], side_sem.at[0, k]),
            pltpu.make_async_copy(high[k], high_own[k], side_sem.at[1, k]),
        )

    for i, (k, p) in enumerate(chunks):
        if p == 0:
            for copy in side(k):
                copy.start()
        load(i).start()

    def region(k, p, origin):
        start, size = rows_of(k, p)
        columns = w[k].shape[1]
        if stacked[k]:
            return out[k].at[origin, pl.ds(start, size)]
        if out[k].shape[1] == columns:
            rows = w[k].shape[0]
            return out[k].at[pl.ds(pl.multiple_of(origin * rows + start, 16), size)]
        return out[k].at[pl.ds(start, size), pl.ds(pl.multiple_of(origin * columns, 128), columns)]

    def hop(i, origin, direction):
        k, p = chunks[i]
        place = region(k, p, origin)
        return pltpu.make_async_remote_copy(
            src_ref=place,
            dst_ref=place,
            send_sem=send_sem.at[direction, origin, i],
            recv_sem=recv_sem.at[direction, origin, i],
            device_id={"rows": z + 1 - 2 * direction},
            device_id_type=MESH,
        )

    def norm_hop(origin, direction):
        return pltpu.make_async_remote_copy(
            src_ref=norm_all.at[origin, t],
            dst_ref=norm_all.at[origin, t],
            send_sem=norm_send.at[direction, origin],
            recv_sem=norm_recv.at[direction, origin],
            device_id={"rows": z + 1 - 2 * direction},
            device_id_type=MESH,
        )

    def cross(step, column):
        return pltpu.make_async_remote_copy(
            src_ref=norm_all.at[:, column],
            dst_ref=norm_all.at[:, column],
            send_sem=cross_send.at[step],
            recv_sem=cross_recv.at[step],
            device_id={"tp": lax.rem(t + step, tps)},
            device_id_type=MESH,
        )

    def send_both(make):
        @pl.when(has_up)
        def _():
            make(0).start()

        @pl.when(has_down)
        def _():
            make(1).start()

    def merge(i):
        k, p = chunks[i]
        start, size = rows_of(k, p)
        columns = w[k].shape[1]
        high_block = block_of(size, (160, 128, 64, 32, 16))
        wide_block = block_of(columns, (256, 128))
        wides = columns // wide_block
        place = region(k, p, z)

        def body(b, _):
            if size == high_block:
                r, c = 0, b
            else:
                r, c = b // wides, b % wides
            r = r * high_block
            c = 0 if wides == 1 else pl.multiple_of(c * wide_block, wide_block)
            mine = pl.ds(start + r, high_block)
            wide = pl.ds(c, wide_block)
            result = w_own[k][mine, wide].astype(jnp.float32) + mix_rate * jnp.dot(
                low_own[k][mine, :], high_own[k][:, wide], preferred_element_type=jnp.float32
            )
            place[pl.ds(r, high_block), wide] = result.astype(jnp.bfloat16)
            return 0

        lax.fori_loop(0, (size // high_block) * wides, body, 0)

    norm = (norm_train[...] + norm_step[...]).astype(jnp.bfloat16).astype(jnp.float32)
    norm_all[z, t] = norm

    for i, (k, p) in enumerate(chunks):
        if p == 0:
            for copy in side(k):
                copy.wait()
        load(i).wait()
        merge(i)
        if i == 0:
            partners = has_up.astype(jnp.int32) + has_down.astype(jnp.int32) + tps - 1
            pl.semaphore_wait(barrier, partners)
        else:
            send_both(functools.partial(hop, i - 1, z))
    send_both(functools.partial(hop, len(chunks) - 1, z))
    send_both(functools.partial(norm_hop, z))

    def arrival(make, d):
        below, above = z - d, z + d

        @pl.when(below >= 0)
        def _():
            make(below, 0).wait_recv()

            @pl.when(has_up)
            def _():
                make(below, 0).start()

        @pl.when(above < n)
        def _():
            make(above, 1).wait_recv()

            @pl.when(has_down)
            def _():
                make(above, 1).start()

    def distance(d, _):
        for i in range(len(chunks)):
            arrival(functools.partial(hop, i), d)
        arrival(norm_hop, d)
        return 0

    def all_norms():
        for step in range(1, tps):
            cross(step, t).start()
        for step in range(1, tps):
            cross(step, lax.rem(t + tps - step, tps)).wait_recv()
        norm_out[...] = jnp.concatenate(
            [norm_all[a, b] for a in range(n) for b in range(tps)], axis=1
        ).astype(jnp.bfloat16)

    lax.fori_loop(1, n, distance, 0)
    all_norms()

    def drain(origin, _):
        for direction, flag in ((0, has_up & (origin <= z)), (1, has_down & (origin >= z))):

            @pl.when(flag)
            def _():
                for i in range(len(chunks)):
                    hop(i, origin, direction).wait_send()
                norm_hop(origin, direction).wait_send()

        return 0

    lax.fori_loop(0, n, drain, 0)
    for step in range(1, tps):
        cross(step, t).wait_send()


def shards(n, tps, *args):
    w, low, high = args[0:12:3], args[1:12:3], args[2:12:3]
    norm_train, norm_step = args[12].reshape(1, -1), args[13].reshape(1, -1)
    kinds = len(w)
    by_column = [False] * (kinds - 1) + [True]
    stacked = [by_column[k] and w[k].shape[1] % 128 != 0 for k in range(kinds)]
    pieces = [pieces_of(*w[k].shape) for k in range(kinds)]
    count = sum(pieces)
    shapes = []
    for k in range(kinds):
        rows, columns = w[k].shape
        if stacked[k]:
            shapes.append((n, rows, columns))
        elif by_column[k]:
            shapes.append((rows, n * columns))
        else:
            shapes.append((n * rows, columns))
    share = norm_train.shape[1]
    vmem, anywhere = pl.BlockSpec(memory_space=pltpu.VMEM), pl.BlockSpec(memory_space=pl.ANY)
    dma = pltpu.SemaphoreType.DMA
    results = pl.pallas_call(
        functools.partial(kernel, n, tps, stacked, pieces),
        out_shape=[jax.ShapeDtypeStruct(s, jnp.bfloat16) for s in shapes]
        + [jax.ShapeDtypeStruct((1, n * tps * share), jnp.bfloat16)],
        in_specs=[anywhere] * (3 * kinds) + [vmem] * 2,
        out_specs=[vmem] * (kinds + 1),
        scratch_shapes=[pltpu.VMEM(x.shape, x.dtype) for x in (*w, *low, *high)]
        + [
            pltpu.VMEM((n, tps, 1, share), jnp.float32),
            dma((count,)),
            dma((2, kinds)),
            dma((2, n, count)),
            dma((2, n, count)),
            dma((2, n)),
            dma((2, n)),
            dma((tps,)),
            dma((tps,)),
        ],
        compiler_params=pltpu.CompilerParams(
            collective_id=0, has_side_effects=True, vmem_limit_bytes=28 * 1024 * 1024
        ),
        name="merge_and_gather",
    )(*w, *low, *high, norm_train, norm_step)
    finals = []
    for k in range(kinds):
        full = results[k]
        if stacked[k]:
            full = full.transpose(1, 0, 2).reshape(full.shape[1], -1)
        finals.append(full)
    return (*finals, results[kinds].reshape(-1))


def solution(mesh):
    return jax.shard_map(
        functools.partial(shards, mesh.shape["rows"], mesh.shape["tp"]),
        mesh=mesh,
        in_specs=(
            P(("unit", "rows"), "tp"),
            P(("unit", "rows"), None),
            P("unit", "tp"),
            P(("unit", "rows"), "tp"),
            P(("unit", "rows"), None),
            P("unit", "tp"),
            P(("unit", "rows"), "tp"),
            P(("unit", "rows"), None),
            P("unit", "tp"),
            P(("unit", "tp"), "rows"),
            P(("unit", "tp"), None),
            P("unit", "rows"),
            P(("unit", "rows", "tp")),
            P(("unit", "rows", "tp")),
        ),
        out_specs=(
            P("unit", "tp"),
            P("unit", "tp"),
            P("unit", "tp"),
            P(("unit", "tp"), None),
            P("unit"),
        ),
        check_vma=False,
    )
```

```python
import functools

import jax
import jax.numpy as jnp
from jax import lax
from jax.experimental import pallas as pl
from jax.experimental.pallas import tpu as pltpu
from jax.sharding import PartitionSpec as P

MESH = pl.DeviceIdType.MESH
mix_rate = 0.5
chunk_bytes = 400 * 1024
first_bytes = 100 * 1024
order = (1, 0, 3, 2)


def pieces_of(rows, columns, most):
    count = 1
    while rows * columns * 2 > count * most and rows % (count * 32) == 0:
        count *= 2
    return count


def block_of(size, options):
    for option in options:
        if size % option == 0:
            return option
    return size


def kernel(n, tps, stacked, pieces, *refs):
    kinds = len(pieces)
    w, low, high = refs[:kinds], refs[kinds : 2 * kinds], refs[2 * kinds : 3 * kinds]
    norm_train, norm_step = refs[3 * kinds : 3 * kinds + 2]
    refs = refs[3 * kinds + 2 :]
    out, norm_out = refs[:kinds], refs[kinds]
    refs = refs[kinds + 1 :]
    w_own, low_own, high_own = refs[:kinds], refs[kinds : 2 * kinds], refs[2 * kinds : 3 * kinds]
    low_rows = refs[3 * kinds : 4 * kinds]
    refs = refs[4 * kinds :]
    norm_own, norm_all, norm_sem, load_sem, side_sem, send_sem, recv_sem, norm_send, norm_recv, cross_send, cross_recv = refs

    z, t = lax.axis_index("rows"), lax.axis_index("tp")
    chunks = [(k, p) for k in order for p in range(pieces[k])]
    has_up, has_down = z < n - 1, z > 0

    barrier = pltpu.get_barrier_semaphore()

    @pl.when(has_up)
    def _():
        pl.semaphore_signal(barrier, inc=1, device_id={"rows": z + 1}, device_id_type=MESH)

    @pl.when(has_down)
    def _():
        pl.semaphore_signal(barrier, inc=1, device_id={"rows": z - 1}, device_id_type=MESH)

    for step in range(1, tps):
        pl.semaphore_signal(barrier, inc=1, device_id={"tp": lax.rem(t + step, tps)}, device_id_type=MESH)

    def rows_of(k, p):
        size = w[k].shape[0] // pieces[k]
        return p * size, size

    def load(i):
        k, p = chunks[i]
        start, size = rows_of(k, p)
        return pltpu.make_async_copy(
            w[k].at[pl.ds(start, size)], w_own[k].at[pl.ds(start, size)], load_sem.at[i]
        )

    def side(k):
        return (
            pltpu.make_async_copy(low[k], low_own[k], side_sem.at[0, k]),
            pltpu.make_async_copy(high[k], high_own[k], side_sem.at[1, k]),
        )

    for i, (k, p) in enumerate(chunks):
        if p == 0:
            for copy in side(k):
                copy.start()
        load(i).start()

    norm_loads = [
        pltpu.make_async_copy(source, norm_own.at[j], norm_sem.at[j])
        for j, source in enumerate((norm_train, norm_step))
    ]
    for copy in norm_loads:
        copy.start()

    def region(k, p, origin):
        start, size = rows_of(k, p)
        columns = w[k].shape[1]
        if stacked[k]:
            return out[k].at[origin, pl.ds(start, size)]
        if out[k].shape[1] == columns:
            rows = w[k].shape[0]
            return out[k].at[pl.ds(pl.multiple_of(origin * rows + start, 16), size)]
        return out[k].at[pl.ds(start, size), pl.ds(pl.multiple_of(origin * columns, 128), columns)]

    def hop(i, origin, direction):
        k, p = chunks[i]
        place = region(k, p, origin)
        return pltpu.make_async_remote_copy(
            src_ref=place,
            dst_ref=place,
            send_sem=send_sem.at[direction, origin, i],
            recv_sem=recv_sem.at[direction, origin, i],
            device_id={"rows": z + 1 - 2 * direction},
            device_id_type=MESH,
        )

    def norm_hop(origin, direction):
        return pltpu.make_async_remote_copy(
            src_ref=norm_all.at[origin, t],
            dst_ref=norm_all.at[origin, t],
            send_sem=norm_send.at[direction, origin],
            recv_sem=norm_recv.at[direction, origin],
            device_id={"rows": z + 1 - 2 * direction},
            device_id_type=MESH,
        )

    def cross(step, column):
        return pltpu.make_async_remote_copy(
            src_ref=norm_all.at[:, column],
            dst_ref=norm_all.at[:, column],
            send_sem=cross_send.at[step],
            recv_sem=cross_recv.at[step],
            device_id={"tp": lax.rem(t + step, tps)},
            device_id_type=MESH,
        )

    def send_both(make):
        @pl.when(has_up)
        def _():
            make(0).start()

        @pl.when(has_down)
        def _():
            make(1).start()

    def merge(i):
        k, p = chunks[i]
        start, size = rows_of(k, p)
        columns = w[k].shape[1]
        high_block = block_of(size, (160, 128, 64, 32, 16))
        wide_block = block_of(columns, (256, 128))
        wides = columns // wide_block
        place = region(k, p, z)

        def body(b, _):
            if size == high_block:
                r, c = 0, b
            else:
                r, c = b // wides, b % wides
            r = r * high_block
            c = 0 if wides == 1 else pl.multiple_of(c * wide_block, wide_block)
            mine = pl.ds(start + r, high_block)
            wide = pl.ds(c, wide_block)
            result = w_own[k][mine, wide].astype(jnp.float32) + mix_rate * jnp.dot(
                low_rows[k][mine, :], high_own[k][:, wide], preferred_element_type=jnp.float32
            )
            place[pl.ds(r, high_block), wide] = result.astype(jnp.bfloat16)
            return 0

        lax.fori_loop(0, (size // high_block) * wides, body, 0)

    for i, (k, p) in enumerate(chunks):
        if p == 0:
            for copy in side(k):
                copy.wait()
            low_rows[k][...] = low_own[k][...].astype(jnp.float32).T.astype(jnp.bfloat16)
        load(i).wait()
        merge(i)
        if i == 0:
            partners = has_up.astype(jnp.int32) + has_down.astype(jnp.int32) + tps - 1
            pl.semaphore_wait(barrier, partners)
        else:
            send_both(functools.partial(hop, i - 1, z))
        if i == 1:
            for copy in norm_loads:
                copy.wait()
            norm_all[z, t] = (norm_own[0] + norm_own[1]).astype(jnp.bfloat16).astype(jnp.float32)
        if i == min(2, len(chunks) - 1):
            send_both(functools.partial(norm_hop, z))
    send_both(functools.partial(hop, len(chunks) - 1, z))

    def arrival(make, d):
        below, above = z - d, z + d

        @pl.when(below >= 0)
        def _():
            make(below, 0).wait_recv()

            @pl.when(has_up)
            def _():
                make(below, 0).start()

        @pl.when(above < n)
        def _():
            make(above, 1).wait_recv()

            @pl.when(has_down)
            def _():
                make(above, 1).start()

    def distance(d, _):
        arrival(norm_hop, d)

        @pl.when(d == n - 1)
        def _():
            for step in range(1, tps):
                cross(step, t).start()

        for i in range(len(chunks)):
            if i == len(chunks) // 2:

                @pl.when(d == n - 1)
                def _():
                    all_norms()

            arrival(functools.partial(hop, i), d)
        return 0

    def all_norms():
        for step in range(1, tps):
            cross(step, lax.rem(t + tps - step, tps)).wait_recv()
        norm_out[...] = jnp.concatenate(
            [norm_all[a, b] for a in range(n) for b in range(tps)], axis=1
        ).astype(jnp.bfloat16)

    lax.fori_loop(1, n, distance, 0)

    def drain(origin, _):
        for direction, flag in ((0, has_up & (origin <= z)), (1, has_down & (origin >= z))):

            @pl.when(flag)
            def _():
                for i in range(len(chunks)):
                    hop(i, origin, direction).wait_send()
                norm_hop(origin, direction).wait_send()

        return 0

    lax.fori_loop(0, n, drain, 0)
    for step in range(1, tps):
        cross(step, t).wait_send()


def put(parts, *refs):
    kinds = len(parts)
    src, dst, sem = refs[:kinds], refs[kinds : 2 * kinds], refs[2 * kinds]
    copies = []
    for k in range(kinds):
        size = src[k].shape[0] // parts[k]
        for p in range(parts[k]):
            rows = pl.ds(p * size, size)
            copies.append(pltpu.make_async_copy(src[k].at[rows], dst[k].at[rows], sem.at[len(copies)]))
    for copy in copies:
        copy.start()
    for copy in copies:
        copy.wait()


def place(arrays):
    parts = [4 if x.shape[0] % 128 == 0 else 1 for x in arrays]
    return pl.pallas_call(
        functools.partial(put, parts),
        out_shape=[jax.ShapeDtypeStruct(x.shape, x.dtype) for x in arrays],
        in_specs=[pl.BlockSpec(memory_space=pltpu.VMEM)] * len(arrays),
        out_specs=[pl.BlockSpec(memory_space=pltpu.HBM)] * len(arrays),
        scratch_shapes=[pltpu.SemaphoreType.DMA((sum(parts),))],
        compiler_params=pltpu.CompilerParams(vmem_limit_bytes=24 * 1024 * 1024),
        name="place",
    )(*arrays)


def shards(n, tps, *args):
    w, low, high = args[0:12:3], [x.T for x in args[1:12:3]], args[2:12:3]
    norm_train, norm_step = args[12].reshape(1, -1), args[13].reshape(1, -1)
    kinds = len(w)
    by_column = [False] * (kinds - 1) + [True]
    stacked = [by_column[k] and w[k].shape[1] % 128 != 0 for k in range(kinds)]
    pieces = [pieces_of(*w[k].shape, first_bytes if k == order[0] else chunk_bytes) for k in range(kinds)]
    count = sum(pieces)
    shapes = []
    for k in range(kinds):
        rows, columns = w[k].shape
        if stacked[k]:
            shapes.append((n, rows, columns))
        elif by_column[k]:
            shapes.append((rows, n * columns))
        else:
            shapes.append((n * rows, columns))
    share = norm_train.shape[1]
    vmem, hbm = pl.BlockSpec(memory_space=pltpu.VMEM), pl.BlockSpec(memory_space=pltpu.HBM)
    dma = pltpu.SemaphoreType.DMA
    operands = (*w, *low, *high, norm_train, norm_step)
    results = pl.pallas_call(
        functools.partial(kernel, n, tps, stacked, pieces),
        out_shape=[pltpu.VMEM(s, jnp.bfloat16) for s in shapes]
        + [pltpu.VMEM((1, n * tps * share), jnp.bfloat16)],
        in_specs=[hbm] * (3 * kinds + 2),
        out_specs=[vmem] * (kinds + 1),
        scratch_shapes=[pltpu.VMEM(x.shape, x.dtype) for x in (*w, *low, *high)]
        + [pltpu.VMEM(x.shape[::-1], x.dtype) for x in low]
        + [
            pltpu.VMEM((2, 1, share), jnp.float32),
            pltpu.VMEM((n, tps, 1, share), jnp.float32),
            dma((2,)),
            dma((count,)),
            dma((2, kinds)),
            dma((2, n, count)),
            dma((2, n, count)),
            dma((2, n)),
            dma((2, n)),
            dma((tps,)),
            dma((tps,)),
        ],
        compiler_params=pltpu.CompilerParams(
            collective_id=0, has_side_effects=True, vmem_limit_bytes=24 * 1024 * 1024
        ),
        name="merge_and_gather",
    )(*[pltpu.with_memory_space_constraint(x, pltpu.HBM) for x in operands])
    results = place(results)
    finals = []
    for k in range(kinds):
        full = results[k]
        if stacked[k]:
            full = full.transpose(1, 0, 2).reshape(full.shape[1], -1)
        finals.append(full)
    return (*finals, results[kinds].reshape(-1))


def solution(mesh):
    return jax.shard_map(
        functools.partial(shards, mesh.shape["rows"], mesh.shape["tp"]),
        mesh=mesh,
        in_specs=(
            P(("unit", "rows"), "tp"),
            P(("unit", "rows"), None),
            P("unit", "tp"),
            P(("unit", "rows"), "tp"),
            P(("unit", "rows"), None),
            P("unit", "tp"),
            P(("unit", "rows"), "tp"),
            P(("unit", "rows"), None),
            P("unit", "tp"),
            P(("unit", "tp"), "rows"),
            P(("unit", "tp"), None),
            P("unit", "rows"),
            P(("unit", "rows", "tp")),
            P(("unit", "rows", "tp")),
        ),
        out_specs=(
            P("unit", "tp"),
            P("unit", "tp"),
            P("unit", "tp"),
            P(("unit", "tp"), None),
            P("unit"),
        ),
        check_vma=False,
    )
```

```python
import functools

import jax
import jax.numpy as jnp
from jax import lax
from jax.experimental import pallas as pl
from jax.experimental.pallas import tpu as pltpu
from jax.sharding import PartitionSpec as P

MESH = pl.DeviceIdType.MESH
mix_rate = 0.5
chunk_bytes = 400 * 1024
first_bytes = 100 * 1024
order = (1, 0, 3, 2)


def pieces_of(rows, columns, most):
    count = 1
    while rows * columns * 2 > count * most and rows % (count * 32) == 0:
        count *= 2
    return count


def block_of(size, options):
    for option in options:
        if size % option == 0:
            return option
    return size


def kernel(n, tps, stacked, pieces, *refs):
    kinds = len(pieces)
    w, low, high = refs[:kinds], refs[kinds : 2 * kinds], refs[2 * kinds : 3 * kinds]
    norm_train, norm_step = refs[3 * kinds : 3 * kinds + 2]
    refs = refs[3 * kinds + 2 :]
    out, norm_out = refs[:kinds], refs[kinds]
    refs = refs[kinds + 1 :]
    w_own, low_own, high_own = refs[:kinds], refs[kinds : 2 * kinds], refs[2 * kinds : 3 * kinds]
    low_rows = refs[3 * kinds : 4 * kinds]
    refs = refs[4 * kinds :]
    norm_own, norm_all, norm_sem, load_sem, side_sem, send_sem, recv_sem, norm_send, norm_recv, cross_send, cross_recv = refs

    z, t = lax.axis_index("rows"), lax.axis_index("tp")
    chunks = [(k, p) for k in order for p in range(pieces[k])]
    has_up, has_down = z < n - 1, z > 0

    def rows_of(k, p):
        size = w[k].shape[0] // pieces[k]
        return p * size, size

    def load(i):
        k, p = chunks[i]
        start, size = rows_of(k, p)
        return pltpu.make_async_copy(
            w[k].at[pl.ds(start, size)], w_own[k].at[pl.ds(start, size)], load_sem.at[i]
        )

    def side(k):
        return (
            pltpu.make_async_copy(low[k], low_own[k], side_sem.at[0, k]),
            pltpu.make_async_copy(high[k], high_own[k], side_sem.at[1, k]),
        )

    def load_kind(kind):
        for copy in side(kind):
            copy.start()
        for i, (k, p) in enumerate(chunks):
            if k == kind:
                load(i).start()

    load_kind(order[0])

    barrier = pltpu.get_barrier_semaphore()

    @pl.when(has_up)
    def _():
        pl.semaphore_signal(barrier, inc=1, device_id={"rows": z + 1}, device_id_type=MESH)

    @pl.when(has_down)
    def _():
        pl.semaphore_signal(barrier, inc=1, device_id={"rows": z - 1}, device_id_type=MESH)

    for step in range(1, tps):
        pl.semaphore_signal(barrier, inc=1, device_id={"tp": lax.rem(t + step, tps)}, device_id_type=MESH)

    for kind in order[1:]:
        load_kind(kind)

    norm_loads = [
        pltpu.make_async_copy(source, norm_own.at[j], norm_sem.at[j])
        for j, source in enumerate((norm_train, norm_step))
    ]
    for copy in norm_loads:
        copy.start()

    def region(k, p, origin):
        start, size = rows_of(k, p)
        columns = w[k].shape[1]
        if stacked[k]:
            return out[k].at[origin, pl.ds(start, size)]
        if out[k].shape[1] == columns:
            rows = w[k].shape[0]
            return out[k].at[pl.ds(pl.multiple_of(origin * rows + start, 16), size)]
        return out[k].at[pl.ds(start, size), pl.ds(pl.multiple_of(origin * columns, 128), columns)]

    def hop(i, origin, direction):
        k, p = chunks[i]
        place = region(k, p, origin)
        return pltpu.make_async_remote_copy(
            src_ref=place,
            dst_ref=place,
            send_sem=send_sem.at[direction, origin, i],
            recv_sem=recv_sem.at[direction, origin, i],
            device_id={"rows": z + 1 - 2 * direction},
            device_id_type=MESH,
        )

    def norm_hop(origin, direction):
        return pltpu.make_async_remote_copy(
            src_ref=norm_all.at[origin, t],
            dst_ref=norm_all.at[origin, t],
            send_sem=norm_send.at[direction, origin],
            recv_sem=norm_recv.at[direction, origin],
            device_id={"rows": z + 1 - 2 * direction},
            device_id_type=MESH,
        )

    def cross(step, column):
        return pltpu.make_async_remote_copy(
            src_ref=norm_all.at[:, column],
            dst_ref=norm_all.at[:, column],
            send_sem=cross_send.at[step],
            recv_sem=cross_recv.at[step],
            device_id={"tp": lax.rem(t + step, tps)},
            device_id_type=MESH,
        )

    def send_both(make):
        @pl.when(has_up)
        def _():
            make(0).start()

        @pl.when(has_down)
        def _():
            make(1).start()

    def merge(i):
        k, p = chunks[i]
        start, size = rows_of(k, p)
        columns = w[k].shape[1]
        high_block = block_of(size, (160, 128, 64, 32, 16))
        wide_block = block_of(columns, (256, 128))
        wides = columns // wide_block
        place = region(k, p, z)

        def body(b, _):
            if size == high_block:
                r, c = 0, b
            else:
                r, c = b // wides, b % wides
            r = r * high_block
            c = 0 if wides == 1 else pl.multiple_of(c * wide_block, wide_block)
            mine = pl.ds(start + r, high_block)
            wide = pl.ds(c, wide_block)
            result = w_own[k][mine, wide].astype(jnp.float32) + mix_rate * jnp.dot(
                low_rows[k][mine, :], high_own[k][:, wide], preferred_element_type=jnp.float32
            )
            place[pl.ds(r, high_block), wide] = result.astype(jnp.bfloat16)
            return 0

        lax.fori_loop(0, (size // high_block) * wides, body, 0)

    for i, (k, p) in enumerate(chunks):
        if p == 0:
            for copy in side(k):
                copy.wait()
            low_rows[k][...] = low_own[k][...].astype(jnp.float32).T.astype(jnp.bfloat16)
        load(i).wait()
        merge(i)
        if i == 1:
            partners = has_up.astype(jnp.int32) + has_down.astype(jnp.int32) + tps - 1
            pl.semaphore_wait(barrier, partners)
        if i > 0:
            send_both(functools.partial(hop, i - 1, z))
        if i == 1:
            for copy in norm_loads:
                copy.wait()
            norm_all[z, t] = (norm_own[0] + norm_own[1]).astype(jnp.bfloat16).astype(jnp.float32)
        if i == min(2, len(chunks) - 1):
            send_both(functools.partial(norm_hop, z))
    send_both(functools.partial(hop, len(chunks) - 1, z))

    def arrival(make, d):
        below, above = z - d, z + d

        @pl.when(below >= 0)
        def _():
            make(below, 0).wait_recv()

            @pl.when(has_up)
            def _():
                make(below, 0).start()

        @pl.when(above < n)
        def _():
            make(above, 1).wait_recv()

            @pl.when(has_down)
            def _():
                make(above, 1).start()

    def distance(d, _):
        arrival(norm_hop, d)

        @pl.when(d == n - 1)
        def _():
            for step in range(1, tps):
                cross(step, t).start()

        for i in range(len(chunks)):
            if i == len(chunks) // 2:

                @pl.when(d == n - 1)
                def _():
                    all_norms()

            arrival(functools.partial(hop, i), d)
        return 0

    def all_norms():
        for step in range(1, tps):
            cross(step, lax.rem(t + tps - step, tps)).wait_recv()
        line = jnp.concatenate([norm_all[a, b] for a in range(n) for b in range(tps)], axis=1)
        width = norm_out.shape[1]
        norm_out[...] = jnp.concatenate(
            [line[:, a * width : (a + 1) * width] for a in range(norm_out.shape[0])], axis=0
        ).astype(jnp.bfloat16)

    lax.fori_loop(1, n, distance, 0)

    def drain(origin, _):
        for direction, flag in ((0, has_up & (origin <= z)), (1, has_down & (origin >= z))):

            @pl.when(flag)
            def _():
                for i in range(len(chunks)):
                    hop(i, origin, direction).wait_send()
                norm_hop(origin, direction).wait_send()

        return 0

    lax.fori_loop(0, n, drain, 0)
    for step in range(1, tps):
        cross(step, t).wait_send()


def put(parts, *refs):
    kinds = len(parts)
    src, dst, sem = refs[:kinds], refs[kinds : 2 * kinds], refs[2 * kinds]
    copies = []
    for k in range(kinds):
        size = src[k].shape[0] // parts[k]
        for p in range(parts[k]):
            rows = pl.ds(p * size, size)
            copies.append(pltpu.make_async_copy(src[k].at[rows], dst[k].at[rows], sem.at[len(copies)]))
    for copy in copies:
        copy.start()
    for copy in copies:
        copy.wait()


def place(arrays):
    parts = [4 if x.shape[0] % 128 == 0 else 1 for x in arrays]
    return pl.pallas_call(
        functools.partial(put, parts),
        out_shape=[jax.ShapeDtypeStruct(x.shape, x.dtype) for x in arrays],
        in_specs=[pl.BlockSpec(memory_space=pltpu.VMEM)] * len(arrays),
        out_specs=[pl.BlockSpec(memory_space=pltpu.HBM)] * len(arrays),
        scratch_shapes=[pltpu.SemaphoreType.DMA((sum(parts),))],
        compiler_params=pltpu.CompilerParams(vmem_limit_bytes=24 * 1024 * 1024),
        name="place",
    )(*arrays)


def shards(n, tps, *args):
    w, low, high = args[0:12:3], [x.T for x in args[1:12:3]], args[2:12:3]
    norm_train, norm_step = args[12].reshape(1, -1), args[13].reshape(1, -1)
    kinds = len(w)
    by_column = [False] * (kinds - 1) + [True]
    stacked = [by_column[k] and w[k].shape[1] % 128 != 0 for k in range(kinds)]
    pieces = [pieces_of(*w[k].shape, first_bytes if k == order[0] else chunk_bytes) for k in range(kinds)]
    count = sum(pieces)
    shapes = []
    for k in range(kinds):
        rows, columns = w[k].shape
        if stacked[k]:
            shapes.append((n, rows, columns))
        elif by_column[k]:
            shapes.append((rows, n * columns))
        else:
            shapes.append((n * rows, columns))
    share = norm_train.shape[1]
    total = n * tps * share
    width = 128 if total % 128 == 0 else total
    vmem, hbm = pl.BlockSpec(memory_space=pltpu.VMEM), pl.BlockSpec(memory_space=pltpu.HBM)
    dma = pltpu.SemaphoreType.DMA
    operands = (*w, *low, *high, norm_train, norm_step)
    results = pl.pallas_call(
        functools.partial(kernel, n, tps, stacked, pieces),
        out_shape=[pltpu.VMEM(s, jnp.bfloat16) for s in shapes]
        + [pltpu.VMEM((total // width, width), jnp.bfloat16)],
        in_specs=[hbm] * (3 * kinds + 2),
        out_specs=[vmem] * (kinds + 1),
        scratch_shapes=[pltpu.VMEM(x.shape, x.dtype) for x in (*w, *low, *high)]
        + [pltpu.VMEM(x.shape[::-1], x.dtype) for x in low]
        + [
            pltpu.VMEM((2, 1, share), jnp.float32),
            pltpu.VMEM((n, tps, 1, share), jnp.float32),
            dma((2,)),
            dma((count,)),
            dma((2, kinds)),
            dma((2, n, count)),
            dma((2, n, count)),
            dma((2, n)),
            dma((2, n)),
            dma((tps,)),
            dma((tps,)),
        ],
        compiler_params=pltpu.CompilerParams(
            collective_id=0, has_side_effects=True, vmem_limit_bytes=24 * 1024 * 1024
        ),
        name="merge_and_gather",
    )(*[pltpu.with_memory_space_constraint(x, pltpu.HBM) for x in operands])
    results = place(results)
    finals = []
    for k in range(kinds):
        full = results[k]
        if stacked[k]:
            full = full.transpose(1, 0, 2).reshape(full.shape[1], -1)
        finals.append(full)
    return (*finals, results[kinds].reshape(-1))


def solution(mesh):
    return jax.shard_map(
        functools.partial(shards, mesh.shape["rows"], mesh.shape["tp"]),
        mesh=mesh,
        in_specs=(
            P(("unit", "rows"), "tp"),
            P(("unit", "rows"), None),
            P("unit", "tp"),
            P(("unit", "rows"), "tp"),
            P(("unit", "rows"), None),
            P("unit", "tp"),
            P(("unit", "rows"), "tp"),
            P(("unit", "rows"), None),
            P("unit", "tp"),
            P(("unit", "tp"), "rows"),
            P(("unit", "tp"), None),
            P("unit", "rows"),
            P(("unit", "rows", "tp")),
            P(("unit", "rows", "tp")),
        ),
        out_specs=(
            P("unit", "tp"),
            P("unit", "tp"),
            P("unit", "tp"),
            P(("unit", "tp"), None),
            P("unit"),
        ),
        check_vma=False,
    )
```

```python
import functools

import jax
import jax.numpy as jnp
from jax import lax
from jax.experimental import pallas as pl
from jax.experimental.pallas import tpu as pltpu
from jax.sharding import PartitionSpec as P

MESH = pl.DeviceIdType.MESH
mix_rate = 0.5
chunk_bytes = 700 * 1024
first_bytes = 100 * 1024
order = (1, 0, 3, 2)


def pieces_of(rows, columns, most):
    count = 1
    while rows * columns * 2 > count * most and rows % (count * 32) == 0:
        count *= 2
    return count


def block_of(size, options):
    for option in options:
        if size % option == 0:
            return option
    return size


def kernel(n, tps, stacked, pieces, *refs):
    kinds = len(pieces)
    w, low, high = refs[:kinds], refs[kinds : 2 * kinds], refs[2 * kinds : 3 * kinds]
    norm_train, norm_step = refs[3 * kinds : 3 * kinds + 2]
    refs = refs[3 * kinds + 2 :]
    out, norm_out = refs[:kinds], refs[kinds]
    refs = refs[kinds + 1 :]
    w_own, low_own, high_own = refs[:kinds], refs[kinds : 2 * kinds], refs[2 * kinds : 3 * kinds]
    low_rows = refs[3 * kinds : 4 * kinds]
    refs = refs[4 * kinds :]
    norm_own, norm_all, norm_sem, load_sem, side_sem, send_sem, recv_sem, pass_send, pass_recv, norm_send, norm_recv, cross_send, cross_recv = refs

    z, t = lax.axis_index("rows"), lax.axis_index("tp")
    chunks = [(k, p) for k in order for p in range(pieces[k])]
    has_up, has_down = z < n - 1, z > 0

    def rows_of(k, p):
        size = w[k].shape[0] // pieces[k]
        return p * size, size

    def load(i):
        k, p = chunks[i]
        start, size = rows_of(k, p)
        return pltpu.make_async_copy(
            w[k].at[pl.ds(start, size)], w_own[k].at[pl.ds(start, size)], load_sem.at[i]
        )

    def side(k):
        return (
            pltpu.make_async_copy(low[k], low_own[k], side_sem.at[0, k]),
            pltpu.make_async_copy(high[k], high_own[k], side_sem.at[1, k]),
        )

    def load_kind(kind):
        for copy in side(kind):
            copy.start()
        for i, (k, p) in enumerate(chunks):
            if k == kind:
                load(i).start()

    load_kind(order[0])

    barrier = pltpu.get_barrier_semaphore()

    @pl.when(has_up)
    def _():
        pl.semaphore_signal(barrier, inc=1, device_id={"rows": z + 1}, device_id_type=MESH)

    @pl.when(has_down)
    def _():
        pl.semaphore_signal(barrier, inc=1, device_id={"rows": z - 1}, device_id_type=MESH)

    for step in range(1, tps):
        pl.semaphore_signal(barrier, inc=1, device_id={"tp": lax.rem(t + step, tps)}, device_id_type=MESH)

    for kind in order[1:]:
        load_kind(kind)

    norm_loads = [
        pltpu.make_async_copy(source, norm_own.at[j], norm_sem.at[j])
        for j, source in enumerate((norm_train, norm_step))
    ]
    for copy in norm_loads:
        copy.start()

    def region(k, p, origin):
        start, size = (0, w[k].shape[0]) if p is None else rows_of(k, p)
        columns = w[k].shape[1]
        if stacked[k]:
            return out[k].at[origin, pl.ds(start, size)]
        if out[k].shape[1] == columns:
            rows = w[k].shape[0]
            return out[k].at[pl.ds(pl.multiple_of(origin * rows + start, 16), size)]
        return out[k].at[pl.ds(start, size), pl.ds(pl.multiple_of(origin * columns, 128), columns)]

    def hop(place, send, recv, direction):
        return pltpu.make_async_remote_copy(
            src_ref=place,
            dst_ref=place,
            send_sem=send,
            recv_sem=recv,
            device_id={"rows": z + 1 - 2 * direction},
            device_id_type=MESH,
        )

    def chunk_hop(i, origin, direction):
        k, p = chunks[i]
        return hop(region(k, p, origin), send_sem.at[direction, i], recv_sem.at[direction, i], direction)

    def whole_hop(k, origin, direction):
        return hop(
            region(k, None, origin),
            pass_send.at[direction, origin, k],
            pass_recv.at[direction, origin, k],
            direction,
        )

    def norm_hop(origin, direction):
        return pltpu.make_async_remote_copy(
            src_ref=norm_all.at[origin, t],
            dst_ref=norm_all.at[origin, t],
            send_sem=norm_send.at[direction, origin],
            recv_sem=norm_recv.at[direction, origin],
            device_id={"rows": z + 1 - 2 * direction},
            device_id_type=MESH,
        )

    def cross(step, column):
        return pltpu.make_async_remote_copy(
            src_ref=norm_all.at[:, column],
            dst_ref=norm_all.at[:, column],
            send_sem=cross_send.at[step],
            recv_sem=cross_recv.at[step],
            device_id={"tp": lax.rem(t + step, tps)},
            device_id_type=MESH,
        )

    def send_both(make):
        @pl.when(has_up)
        def _():
            make(0).start()

        @pl.when(has_down)
        def _():
            make(1).start()

    def merge(i):
        k, p = chunks[i]
        start, size = rows_of(k, p)
        columns = w[k].shape[1]
        high_block = block_of(size, (160, 128, 64, 32, 16))
        wide_block = block_of(columns, (256, 128))
        wides = columns // wide_block
        place = region(k, p, z)

        def body(b, _):
            if size == high_block:
                r, c = 0, b
            else:
                r, c = b // wides, b % wides
            r = r * high_block
            c = 0 if wides == 1 else pl.multiple_of(c * wide_block, wide_block)
            mine = pl.ds(start + r, high_block)
            wide = pl.ds(c, wide_block)
            result = w_own[k][mine, wide].astype(jnp.float32) + mix_rate * jnp.dot(
                low_rows[k][mine, :], high_own[k][:, wide], preferred_element_type=jnp.float32
            )
            place[pl.ds(r, high_block), wide] = result.astype(jnp.bfloat16)
            return 0

        lax.fori_loop(0, (size // high_block) * wides, body, 0)

    for i, (k, p) in enumerate(chunks):
        if p == 0:
            for copy in side(k):
                copy.wait()
            low_rows[k][...] = low_own[k][...].astype(jnp.float32).T.astype(jnp.bfloat16)
        load(i).wait()
        merge(i)
        if i == 1:
            partners = has_up.astype(jnp.int32) + has_down.astype(jnp.int32) + tps - 1
            pl.semaphore_wait(barrier, partners)
        if i > 0:
            send_both(functools.partial(chunk_hop, i - 1, z))
        if i == 1:
            for copy in norm_loads:
                copy.wait()
            norm_all[z, t] = (norm_own[0] + norm_own[1]).astype(jnp.bfloat16).astype(jnp.float32)
        if i == min(2, len(chunks) - 1):
            send_both(functools.partial(norm_hop, z))
    send_both(functools.partial(chunk_hop, len(chunks) - 1, z))

    def arrival(arrived, onward, d):
        below, above = z - d, z + d

        @pl.when(below >= 0)
        def _():
            for make in arrived:
                make(below, 0).wait_recv()

            @pl.when(has_up)
            def _():
                onward(below, 0).start()

        @pl.when(above < n)
        def _():
            for make in arrived:
                make(above, 1).wait_recv()

            @pl.when(has_down)
            def _():
                onward(above, 1).start()

    def distance(d, _, near=False):
        arrival([norm_hop], norm_hop, d)

        @pl.when(d == n - 1)
        def _():
            for step in range(1, tps):
                cross(step, t).start()

        for k in order:
            onward = functools.partial(whole_hop, k)
            arrived = [onward]
            if near:
                arrived = [functools.partial(chunk_hop, i) for i, c in enumerate(chunks) if c[0] == k]
            if k == order[-1]:

                @pl.when(d == n - 1)
                def _():
                    all_norms()

            arrival(arrived, onward, d)
        return 0

    def all_norms():
        for step in range(1, tps):
            cross(step, lax.rem(t + tps - step, tps)).wait_recv()
        line = jnp.concatenate([norm_all[a, b] for a in range(n) for b in range(tps)], axis=1)
        width = norm_out.shape[1]
        norm_out[...] = jnp.concatenate(
            [line[:, a * width : (a + 1) * width] for a in range(norm_out.shape[0])], axis=0
        ).astype(jnp.bfloat16)

    distance(jnp.int32(1), 0, near=True)
    lax.fori_loop(2, n, distance, 0)

    for direction, flag in ((0, has_up), (1, has_down)):

        @pl.when(flag)
        def _():
            for i in range(len(chunks)):
                chunk_hop(i, z, direction).wait_send()
            norm_hop(z, direction).wait_send()

    def drain(origin, _):
        for direction, flag in ((0, has_up & (origin < z)), (1, has_down & (origin > z))):

            @pl.when(flag)
            def _():
                for k in range(kinds):
                    whole_hop(k, origin, direction).wait_send()
                norm_hop(origin, direction).wait_send()

        return 0

    lax.fori_loop(0, n, drain, 0)
    for step in range(1, tps):
        cross(step, t).wait_send()


def put(parts, *refs):
    kinds = len(parts)
    src, dst, sem = refs[:kinds], refs[kinds : 2 * kinds], refs[2 * kinds]
    copies = []
    for k in range(kinds):
        size = src[k].shape[0] // parts[k]
        for p in range(parts[k]):
            rows = pl.ds(p * size, size)
            copies.append(pltpu.make_async_copy(src[k].at[rows], dst[k].at[rows], sem.at[len(copies)]))
    for copy in copies:
        copy.start()
    for copy in copies:
        copy.wait()


def place(arrays):
    parts = [2 if x.shape[0] % 128 == 0 else 1 for x in arrays]
    return pl.pallas_call(
        functools.partial(put, parts),
        out_shape=[jax.ShapeDtypeStruct(x.shape, x.dtype) for x in arrays],
        in_specs=[pl.BlockSpec(memory_space=pltpu.VMEM)] * len(arrays),
        out_specs=[pl.BlockSpec(memory_space=pltpu.HBM)] * len(arrays),
        scratch_shapes=[pltpu.SemaphoreType.DMA((sum(parts),))],
        compiler_params=pltpu.CompilerParams(vmem_limit_bytes=24 * 1024 * 1024),
        name="place",
    )(*arrays)


def shards(n, tps, *args):
    w, low, high = args[0:12:3], [x.T for x in args[1:12:3]], args[2:12:3]
    norm_train, norm_step = args[12].reshape(1, -1), args[13].reshape(1, -1)
    kinds = len(w)
    by_column = [False] * (kinds - 1) + [True]
    stacked = [by_column[k] and w[k].shape[1] % 128 != 0 for k in range(kinds)]
    pieces = [pieces_of(*w[k].shape, first_bytes if k == order[0] else chunk_bytes) for k in range(kinds)]
    count = sum(pieces)
    shapes = []
    for k in range(kinds):
        rows, columns = w[k].shape
        if stacked[k]:
            shapes.append((n, rows, columns))
        elif by_column[k]:
            shapes.append((rows, n * columns))
        else:
            shapes.append((n * rows, columns))
    share = norm_train.shape[1]
    total = n * tps * share
    width = 128 if total % 128 == 0 else total
    vmem, hbm = pl.BlockSpec(memory_space=pltpu.VMEM), pl.BlockSpec(memory_space=pltpu.HBM)
    dma = pltpu.SemaphoreType.DMA
    operands = (*w, *low, *high, norm_train, norm_step)
    results = pl.pallas_call(
        functools.partial(kernel, n, tps, stacked, pieces),
        out_shape=[pltpu.VMEM(s, jnp.bfloat16) for s in shapes]
        + [pltpu.VMEM((total // width, width), jnp.bfloat16)],
        in_specs=[hbm] * (3 * kinds + 2),
        out_specs=[vmem] * (kinds + 1),
        scratch_shapes=[pltpu.VMEM(x.shape, x.dtype) for x in (*w, *low, *high)]
        + [pltpu.VMEM(x.shape[::-1], x.dtype) for x in low]
        + [
            pltpu.VMEM((2, 1, share), jnp.float32),
            pltpu.VMEM((n, tps, 1, share), jnp.float32),
            dma((2,)),
            dma((count,)),
            dma((2, kinds)),
            dma((2, count)),
            dma((2, count)),
            dma((2, n, kinds)),
            dma((2, n, kinds)),
            dma((2, n)),
            dma((2, n)),
            dma((tps,)),
            dma((tps,)),
        ],
        compiler_params=pltpu.CompilerParams(
            collective_id=0, has_side_effects=True, vmem_limit_bytes=24 * 1024 * 1024
        ),
        name="merge_and_gather",
    )(*[pltpu.with_memory_space_constraint(x, pltpu.HBM) for x in operands])
    results = place(results)
    finals = []
    for k in range(kinds):
        full = results[k]
        if stacked[k]:
            full = full.transpose(1, 0, 2).reshape(full.shape[1], -1)
        finals.append(full)
    return (*finals, results[kinds].reshape(-1))


def solution(mesh):
    return jax.shard_map(
        functools.partial(shards, mesh.shape["rows"], mesh.shape["tp"]),
        mesh=mesh,
        in_specs=(
            P(("unit", "rows"), "tp"),
            P(("unit", "rows"), None),
            P("unit", "tp"),
            P(("unit", "rows"), "tp"),
            P(("unit", "rows"), None),
            P("unit", "tp"),
            P(("unit", "rows"), "tp"),
            P(("unit", "rows"), None),
            P("unit", "tp"),
            P(("unit", "tp"), "rows"),
            P(("unit", "tp"), None),
            P("unit", "rows"),
            P(("unit", "rows", "tp")),
            P(("unit", "rows", "tp")),
        ),
        out_specs=(
            P("unit", "tp"),
            P("unit", "tp"),
            P("unit", "tp"),
            P(("unit", "tp"), None),
            P("unit"),
        ),
        check_vma=False,
    )
```

```python
import functools

import jax
import jax.numpy as jnp
from jax import lax
from jax.experimental import pallas as pl
from jax.experimental.pallas import tpu as pltpu
from jax.sharding import PartitionSpec as P

MESH = pl.DeviceIdType.MESH
mix_rate = 0.5
chunk_bytes = 700 * 1024
first_bytes = 200 * 1024
order = (1, 0, 3, 2)


def pieces_of(rows, columns, most):
    count = 1
    while rows * columns * 2 > count * most and rows % (count * 32) == 0:
        count *= 2
    return count


def block_of(size, options):
    for option in options:
        if size % option == 0:
            return option
    return size


def kernel(n, tps, stacked, pieces, *refs):
    kinds = len(pieces)
    w, low, high = refs[:kinds], refs[kinds : 2 * kinds], refs[2 * kinds : 3 * kinds]
    norm_train, norm_step = refs[3 * kinds : 3 * kinds + 2]
    refs = refs[3 * kinds + 2 :]
    out, norm_out = refs[:kinds], refs[kinds]
    refs = refs[kinds + 1 :]
    w_own, low_own, high_own = refs[:kinds], refs[kinds : 2 * kinds], refs[2 * kinds : 3 * kinds]
    low_rows = refs[3 * kinds : 4 * kinds]
    refs = refs[4 * kinds :]
    norm_own, norm_all, norm_sem, load_sem, side_sem, send_sem, recv_sem, pass_send, pass_recv, norm_send, norm_recv, cross_send, cross_recv = refs

    z, t = lax.axis_index("rows"), lax.axis_index("tp")
    chunks = [(k, p) for k in order for p in range(pieces[k])]
    has_up, has_down = z < n - 1, z > 0

    def rows_of(k, p):
        size = w[k].shape[0] // pieces[k]
        return p * size, size

    def load(i):
        k, p = chunks[i]
        start, size = rows_of(k, p)
        return pltpu.make_async_copy(
            w[k].at[pl.ds(start, size)], w_own[k].at[pl.ds(start, size)], load_sem.at[i]
        )

    def side(k):
        return (
            pltpu.make_async_copy(low[k], low_own[k], side_sem.at[0, k]),
            pltpu.make_async_copy(high[k], high_own[k], side_sem.at[1, k]),
        )

    def load_kind(kind):
        for copy in side(kind):
            copy.start()
        for i, (k, p) in enumerate(chunks):
            if k == kind:
                load(i).start()

    load_kind(order[0])

    barrier = pltpu.get_barrier_semaphore()

    @pl.when(has_up)
    def _():
        pl.semaphore_signal(barrier, inc=1, device_id={"rows": z + 1}, device_id_type=MESH)

    @pl.when(has_down)
    def _():
        pl.semaphore_signal(barrier, inc=1, device_id={"rows": z - 1}, device_id_type=MESH)

    for step in range(1, tps):
        pl.semaphore_signal(barrier, inc=1, device_id={"tp": lax.rem(t + step, tps)}, device_id_type=MESH)

    for kind in order[1:]:
        load_kind(kind)

    norm_loads = [
        pltpu.make_async_copy(source, norm_own.at[j], norm_sem.at[j])
        for j, source in enumerate((norm_train, norm_step))
    ]
    for copy in norm_loads:
        copy.start()

    def region(k, p, origin):
        start, size = (0, w[k].shape[0]) if p is None else rows_of(k, p)
        columns = w[k].shape[1]
        if stacked[k]:
            return out[k].at[origin, pl.ds(start, size)]
        if out[k].shape[1] == columns:
            rows = w[k].shape[0]
            return out[k].at[pl.ds(pl.multiple_of(origin * rows + start, 16), size)]
        return out[k].at[pl.ds(start, size), pl.ds(pl.multiple_of(origin * columns, 128), columns)]

    def hop(place, send, recv, direction):
        return pltpu.make_async_remote_copy(
            src_ref=place,
            dst_ref=place,
            send_sem=send,
            recv_sem=recv,
            device_id={"rows": z + 1 - 2 * direction},
            device_id_type=MESH,
        )

    def chunk_hop(i, origin, direction):
        k, p = chunks[i]
        return hop(region(k, p, origin), send_sem.at[direction, i], recv_sem.at[direction, i], direction)

    def whole_hop(k, origin, direction):
        return hop(
            region(k, None, origin),
            pass_send.at[direction, origin, k],
            pass_recv.at[direction, origin, k],
            direction,
        )

    def norm_hop(origin, direction):
        return pltpu.make_async_remote_copy(
            src_ref=norm_all.at[origin, t],
            dst_ref=norm_all.at[origin, t],
            send_sem=norm_send.at[direction, origin],
            recv_sem=norm_recv.at[direction, origin],
            device_id={"rows": z + 1 - 2 * direction},
            device_id_type=MESH,
        )

    def cross(step, column):
        return pltpu.make_async_remote_copy(
            src_ref=norm_all.at[:, column],
            dst_ref=norm_all.at[:, column],
            send_sem=cross_send.at[step],
            recv_sem=cross_recv.at[step],
            device_id={"tp": lax.rem(t + step, tps)},
            device_id_type=MESH,
        )

    def send_both(make):
        @pl.when(has_up)
        def _():
            make(0).start()

        @pl.when(has_down)
        def _():
            make(1).start()

    def merge(i):
        k, p = chunks[i]
        start, size = rows_of(k, p)
        columns = w[k].shape[1]
        high_block = block_of(size, (160, 128, 64, 32, 16))
        wide_block = block_of(columns, (256, 128))
        wides = columns // wide_block
        place = region(k, p, z)

        def body(b, _):
            if size == high_block:
                r, c = 0, b
            else:
                r, c = b // wides, b % wides
            r = r * high_block
            c = 0 if wides == 1 else pl.multiple_of(c * wide_block, wide_block)
            mine = pl.ds(start + r, high_block)
            wide = pl.ds(c, wide_block)
            result = w_own[k][mine, wide].astype(jnp.float32) + mix_rate * jnp.dot(
                low_rows[k][mine, :], high_own[k][:, wide], preferred_element_type=jnp.float32
            )
            place[pl.ds(r, high_block), wide] = result.astype(jnp.bfloat16)
            return 0

        lax.fori_loop(0, (size // high_block) * wides, body, 0)

    for i, (k, p) in enumerate(chunks):
        if p == 0:
            for copy in side(k):
                copy.wait()
            low_rows[k][...] = low_own[k][...].astype(jnp.float32).T.astype(jnp.bfloat16)
        load(i).wait()
        merge(i)
        if i == 1:
            partners = has_up.astype(jnp.int32) + has_down.astype(jnp.int32) + tps - 1
            pl.semaphore_wait(barrier, partners)
        if i > 0:
            send_both(functools.partial(chunk_hop, i - 1, z))
        if i == 1:
            for copy in norm_loads:
                copy.wait()
            norm_all[z, t] = (norm_own[0] + norm_own[1]).astype(jnp.bfloat16).astype(jnp.float32)
        if i == min(2, len(chunks) - 1):
            send_both(functools.partial(norm_hop, z))
    send_both(functools.partial(chunk_hop, len(chunks) - 1, z))

    def arrival(arrived, onward, d):
        below, above = z - d, z + d

        @pl.when(below >= 0)
        def _():
            for make in arrived:
                make(below, 0).wait_recv()

            @pl.when(has_up)
            def _():
                onward(below, 0).start()

        @pl.when(above < n)
        def _():
            for make in arrived:
                make(above, 1).wait_recv()

            @pl.when(has_down)
            def _():
                onward(above, 1).start()

    def distance(d, _, near=False):
        arrival([norm_hop], norm_hop, d)

        @pl.when(d == n - 1)
        def _():
            for step in range(1, tps):
                cross(step, t).start()

        for k in order:
            onward = functools.partial(whole_hop, k)
            arrived = [onward]
            if near:
                arrived = [functools.partial(chunk_hop, i) for i, c in enumerate(chunks) if c[0] == k]
            if k == order[-1]:

                @pl.when(d == n - 1)
                def _():
                    all_norms()

            arrival(arrived, onward, d)
        return 0

    def all_norms():
        for step in range(1, tps):
            cross(step, lax.rem(t + tps - step, tps)).wait_recv()
        line = jnp.concatenate([norm_all[a, b] for a in range(n) for b in range(tps)], axis=1)
        width = norm_out.shape[1]
        norm_out[...] = jnp.concatenate(
            [line[:, a * width : (a + 1) * width] for a in range(norm_out.shape[0])], axis=0
        ).astype(jnp.bfloat16)

    distance(jnp.int32(1), 0, near=True)
    lax.fori_loop(2, n, distance, 0)

    for direction, flag in ((0, has_up), (1, has_down)):

        @pl.when(flag)
        def _():
            for i in range(len(chunks)):
                chunk_hop(i, z, direction).wait_send()
            norm_hop(z, direction).wait_send()

    def drain(origin, _):
        for direction, flag in ((0, has_up & (origin < z)), (1, has_down & (origin > z))):

            @pl.when(flag)
            def _():
                for k in range(kinds):
                    whole_hop(k, origin, direction).wait_send()
                norm_hop(origin, direction).wait_send()

        return 0

    lax.fori_loop(0, n, drain, 0)
    for step in range(1, tps):
        cross(step, t).wait_send()


def put(parts, *refs):
    kinds = len(parts)
    src, dst, sem = refs[:kinds], refs[kinds : 2 * kinds], refs[2 * kinds]
    copies = []
    for k in range(kinds):
        size = src[k].shape[0] // parts[k]
        for p in range(parts[k]):
            rows = pl.ds(p * size, size)
            copies.append(pltpu.make_async_copy(src[k].at[rows], dst[k].at[rows], sem.at[len(copies)]))
    for copy in copies:
        copy.start()
    for copy in copies:
        copy.wait()


def place(arrays):
    parts = [2 if x.shape[0] % 128 == 0 else 1 for x in arrays]
    return pl.pallas_call(
        functools.partial(put, parts),
        out_shape=[jax.ShapeDtypeStruct(x.shape, x.dtype) for x in arrays],
        in_specs=[pl.BlockSpec(memory_space=pltpu.VMEM)] * len(arrays),
        out_specs=[pl.BlockSpec(memory_space=pltpu.HBM)] * len(arrays),
        scratch_shapes=[pltpu.SemaphoreType.DMA((sum(parts),))],
        compiler_params=pltpu.CompilerParams(vmem_limit_bytes=24 * 1024 * 1024),
        name="place",
    )(*arrays)


def shards(n, tps, *args):
    w, low, high = args[0:12:3], [x.T for x in args[1:12:3]], args[2:12:3]
    norm_train, norm_step = args[12].reshape(1, -1), args[13].reshape(1, -1)
    kinds = len(w)
    by_column = [False] * (kinds - 1) + [True]
    stacked = [by_column[k] and w[k].shape[1] % 128 != 0 for k in range(kinds)]
    most = {order[0]: first_bytes, order[1]: chunk_bytes}
    pieces = [pieces_of(*w[k].shape, most.get(k, w[k].size * 2)) for k in range(kinds)]
    count = sum(pieces)
    shapes = []
    for k in range(kinds):
        rows, columns = w[k].shape
        if stacked[k]:
            shapes.append((n, rows, columns))
        elif by_column[k]:
            shapes.append((rows, n * columns))
        else:
            shapes.append((n * rows, columns))
    share = norm_train.shape[1]
    total = n * tps * share
    width = 128 if total % 128 == 0 else total
    vmem, hbm = pl.BlockSpec(memory_space=pltpu.VMEM), pl.BlockSpec(memory_space=pltpu.HBM)
    dma = pltpu.SemaphoreType.DMA
    operands = (*w, *low, *high, norm_train, norm_step)
    results = pl.pallas_call(
        functools.partial(kernel, n, tps, stacked, pieces),
        out_shape=[pltpu.VMEM(s, jnp.bfloat16) for s in shapes]
        + [pltpu.VMEM((total // width, width), jnp.bfloat16)],
        in_specs=[hbm] * (3 * kinds + 2),
        out_specs=[vmem] * (kinds + 1),
        scratch_shapes=[pltpu.VMEM(x.shape, x.dtype) for x in (*w, *low, *high)]
        + [pltpu.VMEM(x.shape[::-1], x.dtype) for x in low]
        + [
            pltpu.VMEM((2, 1, share), jnp.float32),
            pltpu.VMEM((n, tps, 1, share), jnp.float32),
            dma((2,)),
            dma((count,)),
            dma((2, kinds)),
            dma((2, count)),
            dma((2, count)),
            dma((2, n, kinds)),
            dma((2, n, kinds)),
            dma((2, n)),
            dma((2, n)),
            dma((tps,)),
            dma((tps,)),
        ],
        compiler_params=pltpu.CompilerParams(
            collective_id=0, has_side_effects=True, vmem_limit_bytes=24 * 1024 * 1024
        ),
        name="merge_and_gather",
    )(*[pltpu.with_memory_space_constraint(x, pltpu.HBM) for x in operands])
    results = place(results)
    finals = []
    for k in range(kinds):
        full = results[k]
        if stacked[k]:
            full = full.transpose(1, 0, 2).reshape(full.shape[1], -1)
        finals.append(full)
    return (*finals, results[kinds].reshape(-1))


def solution(mesh):
    return jax.shard_map(
        functools.partial(shards, mesh.shape["rows"], mesh.shape["tp"]),
        mesh=mesh,
        in_specs=(
            P(("unit", "rows"), "tp"),
            P(("unit", "rows"), None),
            P("unit", "tp"),
            P(("unit", "rows"), "tp"),
            P(("unit", "rows"), None),
            P("unit", "tp"),
            P(("unit", "rows"), "tp"),
            P(("unit", "rows"), None),
            P("unit", "tp"),
            P(("unit", "tp"), "rows"),
            P(("unit", "tp"), None),
            P("unit", "rows"),
            P(("unit", "rows", "tp")),
            P(("unit", "rows", "tp")),
        ),
        out_specs=(
            P("unit", "tp"),
            P("unit", "tp"),
            P("unit", "tp"),
            P(("unit", "tp"), None),
            P("unit"),
        ),
        check_vma=False,
    )
```
